256 devices in a mesh: dp: 16 (over y, x), sp: 8 (over z), shift: 2 (over core).
Axes of the slice: x: 4, y: 4, z: 8, core: 2. Of those that a mesh axis runs over, the one named last changes fastest.
Arguments:
- query_rows: bfloat16 [32, 2048, 32, 128], P(('shift', 'dp'), 'sp'), parts along dimension 0, may hold values from -6 to 6
- key_rows: bfloat16 [32, 2048, 32, 128], P(('shift', 'dp'), 'sp'), parts along dimension 0, may hold values from -6 to 6
- value_rows: bfloat16 [32, 2048, 32, 128], P(('shift', 'dp'), 'sp'), parts along dimension 0, may hold values from -6 to 6
- out_weight: bfloat16 [8192, 4096], P(('shift', 'dp')), parts along dimension 0, may hold values from -0.09375 to 0.09375
Outputs:
- mixer_out: bfloat16 [32, 2048, 4096], P(('shift', 'dp'), 'sp'), parts along dimension 0
The draws below stay inside these ranges and needn't reach their ends.
There are 2 independent parts, one for each index of `shift`. The reference program is written for one: setup_inputs(seed, part) draws one part's arguments, and reference() takes and returns one part's arrays. A program takes and returns all parts, laid end to end along the dimension named above; each array names one. Nothing has to cross between parts.
All inputs are finite; a program needn't handle non-finite values.
Results may differ from the reference program's by a relative error of at most 0.006.
Values may be sent and summed in bfloat16 or wider, within the bound.
A program may use at most 128 MiB of HBM per device.

```python
import jax
import jax.numpy as jnp
from jax import lax

HEADS = 32
HEAD_SIZE = 128
BATCH = 16
TOKENS = 2048
WIDTH = 4096


def steps_of(key, shape, shards, least, top_value):
    factor_of = 1.0
    for dim, shards_of in shards:
        steps = jax.random.uniform(jax.random.fold_in(jax.random.fold_in(key, 6), dim), (shards_of,), jnp.float32, least / len(shards), top_value / len(shards))
        factor_of = factor_of * jnp.repeat(jnp.exp(steps), shape[dim] // shards_of).reshape((-1,) + (1,) * (len(shape) - 1 - dim))
    return factor_of


def noise(key, dims, scale, most, cuts=(), dtype=jnp.bfloat16):
    entries = jax.random.normal(key, dims, jnp.float32) * scale
    if len(cuts) > 0:
        entries = steps_of(key, dims, cuts, -0.22, 0.18) * entries
    return jnp.clip(entries, min=-most, max=most).astype(dtype)


def setup_inputs(seed: int = 0, part: int = 0) -> dict:
    key_of = jax.random.split(jax.random.key(seed), 5)
    own_keys = jax.random.split(jax.random.fold_in(key_of[4], part), 5)
    return {
        "query_rows": noise(own_keys[0], (BATCH, TOKENS, HEADS, HEAD_SIZE), 1.0, 6.0, ((0, 16), (1, 8))),
        "key_rows": noise(own_keys[1], (BATCH, TOKENS, HEADS, HEAD_SIZE), 1.0, 6.0, ((0, 16), (1, 8))),
        "value_rows": noise(own_keys[2], (BATCH, TOKENS, HEADS, HEAD_SIZE), 1.0, 6.0, ((0, 16), (1, 8))),
        "out_weight": noise(own_keys[3], (WIDTH, WIDTH), WIDTH ** -0.5, 0.09375, ((0, 16),)),
    }


def feature_map(values):
    wide = values.astype(jnp.float32)
    return (jnp.where(wide > 0.0, wide + 1.0, jnp.exp(jnp.minimum(wide, 0.0)))).astype(jnp.bfloat16)


def finish_heads(read, count):
    result = read * count ** 0.5
    return result.astype(jnp.bfloat16)


def ask_state(features, state, mass):
    small = lax.optimization_barrier(state.astype(jnp.bfloat16))
    top = jnp.einsum("bthd,bhde->bthe", features.astype(jnp.float32), small.astype(jnp.float32))
    bottom = jnp.einsum("bthd,bhd->bth", features.astype(jnp.float32), mass, precision=lax.Precision.HIGHEST)
    return top / (bottom + 1e-3)[..., None]


def reference(query_rows, key_rows, value_rows, out_weight):
    query_feature, key_feature = lax.optimization_barrier((feature_map(query_rows), feature_map(key_rows)))
    state = jnp.einsum("bthd,bthe->bhde", key_feature.astype(jnp.float32), value_rows.astype(jnp.float32)) / TOKENS
    mass = jnp.sum(key_feature.astype(jnp.float32), axis=1) / TOKENS
    mixed = finish_heads(ask_state(query_feature, state, mass), TOKENS).reshape(BATCH, TOKENS, WIDTH)
    mixed = lax.optimization_barrier(mixed)
    mixer_out = jnp.einsum("btw,wv->btv", mixed.astype(jnp.float32), out_weight.astype(jnp.float32)).astype(jnp.bfloat16)
    return mixer_out
```

```python
import functools

import jax
import jax.numpy as jnp
from jax import lax
from jax.experimental import pallas as pl
from jax.experimental.pallas import tpu as pltpu
from jax.sharding import PartitionSpec as P

MESH = pl.DeviceIdType.MESH
RING = 4
DEPTH = 8
HEADS = 32
SIZE = 128
TOKENS = 256
NEAR = 128
ROWS = TOKENS + 2 * NEAR
BLOCK = 256
WIDTH = 4096
PITCH = 40
WAVES = (512, 512)
STARTS = (0, 1024)
PAIRS = HEADS // 2
SUMS = 2 * SIZE + 8
SENT = 2 * SIZE + 32
F32 = jnp.float32
BF16 = jnp.bfloat16


def feature(values):
    return jnp.where(values > 0.0, values + 1.0, jnp.exp(jnp.minimum(values, 0.0)))


def kernel(
    q_hbm,
    k_hbm,
    v_hbm,
    w_hbm,
    out_hbm,
    w0,
    w1,
    k_in,
    v_in,
    near,
    wide,
    part,
    from_left,
    from_right,
    held,
    mixed,
    acc,
    done0,
    done1,
    local_sem,
    send_sem,
    recv_sem,
):
    dp = lax.axis_index("dp")
    z = lax.axis_index("sp")
    y, x = dp // RING, dp % RING
    half = z % 2
    weights, done = (w0, w1), (done0, done1)

    def z_dev(step):
        return {"sp": (z + step + DEPTH) % DEPTH}

    def flat_dev(along, step):
        if along == "x":
            return {"dp": y * RING + (x + step + RING) % RING}
        return {"dp": ((y + step + RING) % RING) * RING + x}

    ids = {}
    sent = []

    def message(key, src, dst, device):
        i = ids.setdefault(key, len(ids))
        return pltpu.make_async_remote_copy(
            src_ref=src,
            dst_ref=dst,
            send_sem=send_sem.at[i],
            recv_sem=recv_sem.at[i],
            device_id=device,
            device_id_type=MESH,
        )

    def send(key, src, dst, device):
        copy = message(key, src, dst, device)
        copy.start()
        sent.append(copy)

    def receive(key, ref, device):
        message(key, ref, ref, device).wait_recv()

    firsts, seconds = ("x", "y"), ("y", "x")
    f_at, g_at = (x, y), (y, x)

    def block(t, wave, df, dg, rows=None):
        f = (f_at[t] + df + RING) % RING
        g = (g_at[t] + dg + RING) % RING
        start = pl.multiple_of((g * RING + f) * BLOCK, BLOCK)
        if rows is None:
            return weights[wave].at[t, pl.ds(start, BLOCK), :]
        return weights[wave].at[t, pl.ds(pl.multiple_of(start + rows * (BLOCK // 2), BLOCK // 2), BLOCK // 2), :]

    def send_first(t, wave):
        for d in (1, -1):
            ref = block(t, wave, 0, 0)
            send(("first", t, wave, d), ref, ref, flat_dev(firsts[t], d))

    def take_first(t, wave, d):
        receive(("first", t, wave, d), block(t, wave, -d, 0), flat_dev(firsts[t], d))

    def send_first_half(t, wave, d):
        ref = block(t, wave, -d, 0, 0 if d == 1 else 1)
        send(("first half", t, wave, d), ref, ref, flat_dev(firsts[t], d))

    def take_first_half(t, wave, d):
        receive(("first half", t, wave, d), block(t, wave, -2 * d, 0, 0 if d == 1 else 1), flat_dev(firsts[t], d))

    def send_second(t, wave, j):
        for d in (1, -1):
            ref = block(t, wave, j, 0)
            send(("second", t, wave, d, j), ref, ref, flat_dev(seconds[t], d))

    def pass_second(t, wave, j):
        for d in (1, -1):
            receive(("second", t, wave, d, j), block(t, wave, j, -d), flat_dev(seconds[t], d))
            ref = block(t, wave, j, -d, 0 if d == 1 else 1)
            send(("second half", t, wave, d, j), ref, ref, flat_dev(seconds[t], d))

    def take_second_half(t, wave, j):
        for d in (1, -1):
            ref = block(t, wave, j, -2 * d, 0 if d == 1 else 1)
            receive(("second half", t, wave, d, j), ref, flat_dev(seconds[t], d))

    def gather_1(wave):
        for t in (0, 1):
            for d in (1, -1):
                take_first(t, wave, d)
                send_first_half(t, wave, d)
        for j in (-1, 1):
            for t in (0, 1):
                send_second(t, wave, j)

    def gather_2(wave):
        for t in (0, 1):
            for d in (1, -1):
                take_first_half(t, wave, d)
        for t in (0, 1):
            send_second(t, wave, 2)

    def gather_3(wave, j):
        for t in (0, 1):
            pass_second(t, wave, j)

    def gather_4(wave):
        for j in (0, -1, 1, 2):
            for t in (0, 1):
                take_second_half(t, wave, j)

    loads = []
    for wave in (0, 1):
        for t in (0, 1):
            start = pl.multiple_of(half * (WIDTH // 2) + STARTS[wave] + t * WAVES[wave], 128)
            loads.append(
                pltpu.make_async_copy(
                    w_hbm.at[:, pl.ds(start, WAVES[wave])], block(t, wave, 0, 0), local_sem.at[2 * wave + t]
                )
            )
    k_load = pltpu.make_async_copy(k_hbm, k_in, local_sem.at[4])
    v_load = pltpu.make_async_copy(v_hbm, v_in, local_sem.at[5])
    for load in loads:
        load.start()
    k_load.start()
    v_load.start()

    barrier = pltpu.get_barrier_semaphore()
    around = [flat_dev("x", 1), flat_dev("x", -1), flat_dev("y", 1), flat_dev("y", -1), z_dev(1), z_dev(-1)]
    for device in around:
        pl.semaphore_signal(barrier, inc=1, device_id=device, device_id_type=MESH)
    pl.semaphore_wait(barrier, len(around))

    for wave in (0,):
        for t in (0, 1):
            loads[2 * wave + t].wait()
        for t in (0, 1):
            send_first(t, wave)
        for t in (0, 1):
            send_second(t, wave, 0)
    send(("q", 1), q_hbm.at[pl.ds(NEAR * HEADS, NEAR * HEADS), :], near.at[0], z_dev(1))
    send(("q", -1), q_hbm.at[pl.ds(0, NEAR * HEADS), :], near.at[1], z_dev(-1))

    def widen(src, at, count, fn):
        def step(i, carry):
            for u in range(4):
                row = pl.multiple_of((i * 4 + u) * HEADS, HEADS)
                to = pl.multiple_of((at + i * 4 + u) * PITCH, 8)
                wide[pl.ds(to, HEADS), :] = fn(src(row))
            return carry

        lax.fori_loop(0, count // 4, step, 0)

    def as_feature(values):
        return feature(values.astype(F32)).astype(BF16).astype(F32)

    k_load.wait()
    widen(lambda row: k_in[pl.ds(row, HEADS), :], 0, TOKENS, as_feature)
    q_load = pltpu.make_async_copy(q_hbm, k_in, local_sem.at[6])
    q_load.start()
    v_load.wait()
    widen(lambda row: v_in[pl.ds(row, HEADS), :], TOKENS, TOKENS, lambda values: values.astype(F32))

    gather_1(0)

    sub = lax.broadcasted_iota(jnp.int32, (8, SIZE), 0)

    def states(i, carry):
        masses = []
        for u in (0, 1):
            head = 2 * i + u
            keys = wide[pl.ds(head, TOKENS, stride=PITCH), :]
            values = wide[pl.ds(TOKENS * PITCH + head, TOKENS, stride=PITCH), :]
            part[i, pl.ds(u * SIZE, SIZE), :] = lax.dot_general(
                keys.astype(BF16), values.astype(BF16), (((0,), (0,)), ((), ())), preferred_element_type=F32
            )
            masses.append(jnp.sum(keys, axis=0, keepdims=True))
        part[i, pl.ds(2 * SIZE, 8), :] = jnp.where(sub == 0, masses[0], jnp.where(sub == 1, masses[1], 0.0))
        return carry

    lax.fori_loop(0, PAIRS, states, 0)

    def at(chunk, u):
        return ((chunk + 2 * DEPTH) % DEPTH) * 2 + u

    lands = {1: from_left, -1: from_right}

    def reduce_send(d, step, u):
        send(("sum", d, step, u), part.at[at(z + d * (5 - step), u)], lands[d].at[2 * (step - 1) + u], z_dev(d))

    def reduce_add(d, step, u):
        slot = 2 * (step - 1) + u
        receive(("sum", d, step, u), lands[d].at[slot], z_dev(d))
        mine = at(z + d * (4 - step), u)
        part[mine] = part[mine] + lands[d][slot]

    for d, u in ((1, 0), (-1, 1)):
        reduce_send(d, 1, u)
    for d, u in ((1, 1), (-1, 0)):
        reduce_send(d, 2, u)

    for wave in (1,):
        for t in (0, 1):
            loads[2 * wave + t].wait()
        for t in (0, 1):
            send_first(t, wave)
        for t in (0, 1):
            send_second(t, wave, 0)

    q_load.wait()
    widen(lambda row: k_in[pl.ds(row, HEADS), :], 0, TOKENS, as_feature)
    gather_2(0)
    gather_3(0, 0)

    for d, u in ((1, 0), (-1, 1)):
        reduce_add(d, 1, u)
        reduce_send(d, 2, u)

    for slot, (d, first) in enumerate(((1, NEAR), (-1, 0))):
        receive(("q", d), near.at[slot], z_dev(d))
        widen(lambda row, slot=slot: near[slot, pl.ds(row, HEADS), :], TOKENS + slot * NEAR, NEAR, as_feature)
    gather_3(0, -1)

    for u in (1, 0):
        for d in (1, -1):
            v = u if d == 1 else 1 - u
            reduce_add(d, 2, v)
            reduce_send(d, 3, v)
    gather_3(0, 1)
    gather_1(1)

    for u in (1, 0):
        for d in (1, -1):
            v = u if d == 1 else 1 - u
            reduce_add(d, 3, v)
            reduce_send(d, 4, v)
    gather_3(0, 2)

    def gather_send(d, step, u):
        ref = held.at[at(z - d * (step - 1), u)]
        send(("state", d, step, u), ref, ref, z_dev(d))

    def gather_take(d, step, u):
        receive(("state", d, step, u), held.at[at(z - d * step, u)], z_dev(d))

    def read_pair(i):
        terms = held[i, pl.ds(2 * SIZE, 32), :].astype(F32)
        block_at = i
        other_at = (i % RING) * RING + i // RING
        for u in (0, 1):
            head = 2 * i + u
            mass = terms[u : u + 1] + terms[8 + u : 9 + u] + terms[16 + u : 17 + u]
            state = held[i, pl.ds(u * SIZE, SIZE), :]
            for r in range(0, ROWS, 256):
                ask = wide[pl.ds(r * PITCH + head, 256, stride=PITCH), :]
                bottom = jnp.sum(ask * mass, axis=1, keepdims=True) + 0.001
                top = jnp.dot(ask.astype(BF16), state, preferred_element_type=F32)
                result = (top * (2048.0**0.5 / bottom)).astype(BF16)
                for t, b in ((0, block_at), (1, other_at)):
                    to = pl.multiple_of(b * BLOCK + u * SIZE, SIZE)
                    mixed[t, pl.ds(r, 256), pl.ds(to, SIZE)] = result

    def read_chunk(chunk, subs):
        first, count = subs

        def step(j, carry):
            read_pair(at(chunk, 0) + first + j)
            return carry

        lax.fori_loop(0, count, step, 0)

    mine = at(z, 0)
    for u in (0, 1):
        for d in (1, -1):
            receive(("sum", d, 4, u), lands[d].at[6 + u], z_dev(d))
        total = (part[mine + u] + from_left[6 + u] + from_right[6 + u]) * (1.0 / 2048.0)
        held[mine + u, pl.ds(0, 2 * SIZE), :] = total[: 2 * SIZE].astype(BF16)
        mass = total[2 * SIZE :]
        high = mass.astype(BF16).astype(F32)
        middle = (mass - high).astype(BF16).astype(F32)
        low = mass - high - middle
        terms = jnp.concatenate([high, middle, low, jnp.zeros_like(low)], axis=0)
        held[mine + u, pl.ds(2 * SIZE, 32), :] = terms.astype(BF16)
        for d in (1, -1):
            gather_send(d, 1, u)

    read_chunk(z, (0, 2))
    gather_4(0)
    for step in (1, 2, 3):
        for u in (0, 1):
            for d in (1, -1):
                gather_take(d, step, u)
                if step < 3 or (u == 0) == (d == 1):
                    gather_send(d, step + 1, u)
        if step == 2:
            gather_3(1, 0)
        for d in (1, -1):
            read_chunk(z - d * step, (0, 2))
    gather_2(1)
    gather_take(1, 4, 0)
    gather_take(-1, 4, 1)
    read_chunk(z + 4, (0, 2))

    gather_3(1, -1)

    out_at = [half * (WIDTH // 2) + start for start in STARTS]
    own_stores = []

    def finish(wave, rows_at):
        columns = 2 * WAVES[wave]
        start = pl.multiple_of(out_at[wave], 128)
        if rows_at == TOKENS:
            send(
                ("out", wave, -1),
                done[wave].at[pl.ds(TOKENS, NEAR), :],
                out_hbm.at[pl.ds(NEAR, NEAR), pl.ds(start, columns)],
                z_dev(-1),
            )
            send(
                ("out", wave, 1),
                done[wave].at[pl.ds(TOKENS + NEAR, NEAR), :],
                out_hbm.at[pl.ds(0, NEAR), pl.ds(start, columns)],
                z_dev(1),
            )
        else:
            copy = pltpu.make_async_copy(
                done[wave].at[pl.ds(0, TOKENS), :],
                out_hbm.at[pl.ds(0, TOKENS), pl.ds(start, columns)],
                local_sem.at[7 + wave],
            )
            copy.start()
            own_stores.append(copy)

    TILE = 256

    def multiply(wave, rows_at, groups, first, last):
        for t in (0, 1):

            def step(n, carry, t=t):
                column = pl.multiple_of(n * TILE, TILE)
                to = pl.multiple_of(t * WAVES[wave] + n * TILE, TILE)
                rows = pl.ds(rows_at, 256)
                total = None if first else acc[rows, pl.ds(to, TILE)]
                if groups is None:
                    total = jnp.dot(
                        mixed[t, rows, :], weights[wave][t, :, pl.ds(column, TILE)], preferred_element_type=F32
                    )
                else:
                    for dg in groups:
                        g = (g_at[t] + dg + RING) % RING
                        depth = pl.ds(pl.multiple_of(g * RING * BLOCK, RING * BLOCK), RING * BLOCK)
                        product = jnp.dot(
                            mixed[t, rows, depth],
                            weights[wave][t, depth, pl.ds(column, TILE)],
                            preferred_element_type=F32,
                        )
                        total = product if total is None else total + product
                if last:
                    done[wave][rows, pl.ds(to, TILE)] = total.astype(BF16)
                else:
                    acc[rows, pl.ds(to, TILE)] = total
                return carry

            lax.fori_loop(0, WAVES[wave] // TILE, step, 0)

    multiply(0, TOKENS, None, True, True)
    finish(0, TOKENS)
    gather_3(1, 1)
    multiply(0, 0, None, True, True)
    finish(0, 0)
    gather_3(1, 2)
    for rows_at in (TOKENS, 0):
        multiply(1, rows_at, (0, -1, 1), True, False)
    gather_4(1)
    for rows_at in (TOKENS, 0):
        multiply(1, rows_at, (2,), False, True)
        finish(1, rows_at)

    for copy in own_stores:
        copy.wait()
    for copy in sent:
        copy.wait_send()
    for wave in (0, 1):
        columns = 2 * WAVES[wave]
        start = pl.multiple_of((1 - half) * (WIDTH // 2) + STARTS[wave], 128)
        receive(("out", wave, -1), out_hbm.at[pl.ds(NEAR, NEAR), pl.ds(start, columns)], z_dev(-1))
        receive(("out", wave, 1), out_hbm.at[pl.ds(0, NEAR), pl.ds(start, columns)], z_dev(1))
    assert len(ids) <= MESSAGES, len(ids)


MESSAGES = 114


def body(query_rows, key_rows, value_rows, out_weight):
    rows = [a.reshape(TOKENS * HEADS, SIZE) for a in (query_rows, key_rows, value_rows)]
    anywhere = pl.BlockSpec(memory_space=pltpu.HBM)
    result = pl.pallas_call(
        kernel,
        out_shape=jax.ShapeDtypeStruct((TOKENS, WIDTH), BF16),
        in_specs=[anywhere] * 4,
        out_specs=anywhere,
        scratch_shapes=[
            pltpu.VMEM((2, WIDTH, WAVES[0]), BF16),
            pltpu.VMEM((2, WIDTH, WAVES[1]), BF16),
            pltpu.VMEM((TOKENS * HEADS, SIZE), BF16),
            pltpu.VMEM((TOKENS * HEADS, SIZE), BF16),
            pltpu.VMEM((2, NEAR * HEADS, SIZE), BF16),
            pltpu.VMEM((ROWS * PITCH, SIZE), F32),
            pltpu.VMEM((PAIRS, SUMS, SIZE), F32),
            pltpu.VMEM((8, SUMS, SIZE), F32),
            pltpu.VMEM((8, SUMS, SIZE), F32),
            pltpu.VMEM((PAIRS, SENT, SIZE), BF16),
            pltpu.VMEM((2, ROWS, WIDTH), BF16),
            pltpu.VMEM((ROWS, 2 * WAVES[1]), F32),
            pltpu.VMEM((ROWS, 2 * WAVES[0]), BF16),
            pltpu.VMEM((ROWS, 2 * WAVES[1]), BF16),
            pltpu.SemaphoreType.DMA((9,)),
            pltpu.SemaphoreType.DMA((MESSAGES,)),
            pltpu.SemaphoreType.DMA((MESSAGES,)),
        ],
        compiler_params=pltpu.CompilerParams(
            collective_id=0, has_side_effects=True, vmem_limit_bytes=60 * 1024 * 1024
        ),
        name="attend",
    )(*rows, out_weight)
    return result.reshape(1, TOKENS, WIDTH)


def solution(mesh):
    placed = (
        P(("shift", "dp"), "sp", None, None),
        P(("shift", "dp"), "sp", None, None),
        P(("shift", "dp"), "sp", None, None),
        P(("shift", "dp"), None),
    )
    return jax.shard_map(
        body, mesh=mesh, in_specs=placed, out_specs=P(("shift", "dp"), "sp", None), check_vma=False
    )
```

```python
import jax
import jax.numpy as jnp
from jax import lax
from jax.experimental import pallas as pl
from jax.experimental.pallas import tpu as pltpu
from jax.sharding import PartitionSpec as P

MESH = pl.DeviceIdType.MESH
RING = 4
DEPTH = 8
HEADS = 32
SIZE = 128
TOKENS = 256
NEAR = 128
OWN = 2 * NEAR
ROWS = TOKENS + OWN
BLOCK = 256
WIDTH = 4096
PITCH = 40
WAVES = (768, 128, 128)
STARTS = tuple(2 * sum(WAVES[:i]) for i in range(len(WAVES)))
PAIRS = HEADS // 2
SUMS = 2 * SIZE + 8
SENT = 2 * SIZE + 32
F32 = jnp.float32
BF16 = jnp.bfloat16


def feature(values):
    return jnp.where(values > 0.0, values + 1.0, jnp.exp(jnp.minimum(values, 0.0)))


def kernel(q_hbm, k_hbm, v_hbm, w_hbm, out, *scratch):
    weights, scratch = scratch[: len(WAVES)], scratch[len(WAVES) :]
    accs, scratch = scratch[: len(WAVES)], scratch[len(WAVES) :]
    done, scratch = scratch[: len(WAVES)], scratch[len(WAVES) :]
    k_in, v_in, near, wide, part, from_left, from_right, held, mixed, local_sem, send_sem, recv_sem = scratch
    dp = lax.axis_index("dp")
    z = lax.axis_index("sp")
    y, x = dp // RING, dp % RING
    half = z % 2

    def z_dev(step):
        return {"sp": (z + step + DEPTH) % DEPTH}

    def flat_dev(along, step):
        if along == "x":
            return {"dp": y * RING + (x + step + RING) % RING}
        return {"dp": ((y + step + RING) % RING) * RING + x}

    ids = {}
    sent = []

    def message(key, src, dst, device):
        i = ids.setdefault(key, len(ids))
        return pltpu.make_async_remote_copy(
            src_ref=src,
            dst_ref=dst,
            send_sem=send_sem.at[i],
            recv_sem=recv_sem.at[i],
            device_id=device,
            device_id_type=MESH,
        )

    def send(key, src, dst, device):
        copy = message(key, src, dst, device)
        copy.start()
        sent.append(copy)

    def receive(key, ref, device):
        message(key, ref, ref, device).wait_recv()

    firsts, seconds = ("x", "y"), ("y", "x")
    f_at, g_at = (x, y), (y, x)

    def block(t, wave, df, dg, rows=None):
        f = (f_at[t] + df + RING) % RING
        g = (g_at[t] + dg + RING) % RING
        start = pl.multiple_of((g * RING + f) * BLOCK, BLOCK)
        if rows is None:
            return weights[wave].at[t, pl.ds(start, BLOCK), :]
        return weights[wave].at[t, pl.ds(pl.multiple_of(start + rows * (BLOCK // 2), BLOCK // 2), BLOCK // 2), :]

    def send_first(t, wave):
        for d in (1, -1):
            ref = block(t, wave, 0, 0)
            send(("first", t, wave, d), ref, ref, flat_dev(firsts[t], d))

    def take_first(t, wave, d):
        receive(("first", t, wave, d), block(t, wave, -d, 0), flat_dev(firsts[t], d))

    def send_first_half(t, wave, d):
        ref = block(t, wave, -d, 0, 0 if d == 1 else 1)
        send(("first half", t, wave, d), ref, ref, flat_dev(firsts[t], d))

    def take_first_half(t, wave, d):
        receive(("first half", t, wave, d), block(t, wave, -2 * d, 0, 0 if d == 1 else 1), flat_dev(firsts[t], d))

    def send_second(t, wave, j):
        for d in (1, -1):
            ref = block(t, wave, j, 0)
            send(("second", t, wave, d, j), ref, ref, flat_dev(seconds[t], d))

    def pass_second(t, wave, j):
        for d in (1, -1):
            receive(("second", t, wave, d, j), block(t, wave, j, -d), flat_dev(seconds[t], d))
            ref = block(t, wave, j, -d, 0 if d == 1 else 1)
            send(("second half", t, wave, d, j), ref, ref, flat_dev(seconds[t], d))

    def take_second_half(t, wave, j):
        for d in (1, -1):
            ref = block(t, wave, j, -2 * d, 0 if d == 1 else 1)
            receive(("second half", t, wave, d, j), ref, flat_dev(seconds[t], d))

    def gather_1(wave):
        for t in (0, 1):
            for d in (1, -1):
                take_first(t, wave, d)
                send_first_half(t, wave, d)
        for j in (-1, 1):
            for t in (0, 1):
                send_second(t, wave, j)

    def gather_2(wave):
        for t in (0, 1):
            for d in (1, -1):
                take_first_half(t, wave, d)
        for t in (0, 1):
            send_second(t, wave, 2)

    def gather_3(wave, j):
        for t in (0, 1):
            pass_second(t, wave, j)

    def gather_4(wave):
        for j in (0, -1, 1, 2):
            for t in (0, 1):
                take_second_half(t, wave, j)

    barrier = pltpu.get_barrier_semaphore()
    around = [flat_dev("x", 1), flat_dev("x", -1), flat_dev("y", 1), flat_dev("y", -1), z_dev(1), z_dev(-1)]
    for device in around:
        pl.semaphore_signal(barrier, inc=1, device_id=device, device_id_type=MESH)
    loads = []
    for wave in range(len(WAVES)):
        for t in (0, 1):
            start = pl.multiple_of(half * (WIDTH // 2) + STARTS[wave] + t * WAVES[wave], 128)
            loads.append(
                pltpu.make_async_copy(
                    w_hbm.at[:, pl.ds(start, WAVES[wave])], block(t, wave, 0, 0), local_sem.at[2 * wave + t]
                )
            )
    k_load = pltpu.make_async_copy(k_hbm, k_in, local_sem.at[2 * len(WAVES)])
    v_load = pltpu.make_async_copy(v_hbm, v_in, local_sem.at[2 * len(WAVES) + 1])
    q_load = pltpu.make_async_copy(q_hbm, k_in, local_sem.at[2 * len(WAVES) + 2])
    for load in loads[:2] + [k_load, v_load] + loads[2:]:
        load.start()
    pl.semaphore_wait(barrier, len(around))

    def send_own(wave):
        for t in (0, 1):
            loads[2 * wave + t].wait()
        for t in (0, 1):
            send_first(t, wave)
        for t in (0, 1):
            send_second(t, wave, 0)

    QUARTER = NEAR // 2

    def near_rows(d, late):
        row = (0 if d == 1 else NEAR) + (QUARTER if late == (d == -1) else 0)
        return near.at[pl.ds(row * HEADS, QUARTER * HEADS), :], row

    def send_queries(late):
        for d in (1, -1):
            position = {(1, True): NEAR, (1, False): NEAR + QUARTER, (-1, False): 0, (-1, True): QUARTER}[d, late]
            ref, _ = near_rows(d, late)
            send(("q", d, late), q_hbm.at[pl.ds(position * HEADS, QUARTER * HEADS), :], ref, z_dev(d))

    send_own(0)
    send_queries(False)

    def widen(src, at, count, fn):
        def step(i, carry):
            for u in range(4):
                row = pl.multiple_of((i * 4 + u) * HEADS, HEADS)
                to = pl.multiple_of((at + i * 4 + u) * PITCH, 8)
                wide[pl.ds(to, HEADS), :] = fn(src(row))
            return carry

        lax.fori_loop(0, count // 4, step, 0)

    def as_feature(values):
        return feature(values.astype(F32)).astype(BF16).astype(F32)

    k_load.wait()
    widen(lambda row: k_in[pl.ds(row, HEADS), :], 0, TOKENS, as_feature)
    q_load.start()
    v_load.wait()
    widen(lambda row: v_in[pl.ds(row, HEADS), :], TOKENS, TOKENS, lambda values: values.astype(F32))

    sub = lax.broadcasted_iota(jnp.int32, (8, SIZE), 0)

    def states(i, carry):
        masses = []
        for u in (0, 1):
            head = 2 * i + u
            keys = wide[pl.ds(head, TOKENS, stride=PITCH), :]
            values = wide[pl.ds(TOKENS * PITCH + head, TOKENS, stride=PITCH), :]
            part[i, pl.ds(u * SIZE, SIZE), :] = lax.dot_general(
                keys.astype(BF16), values.astype(BF16), (((0,), (0,)), ((), ())), preferred_element_type=F32
            )
            masses.append(jnp.sum(keys, axis=0, keepdims=True))
        part[i, pl.ds(2 * SIZE, 8), :] = jnp.where(sub == 0, masses[0], jnp.where(sub == 1, masses[1], 0.0))
        return carry

    lax.fori_loop(0, PAIRS, states, 0)

    def at(chunk, u):
        return ((chunk + 2 * DEPTH) % DEPTH) * 2 + u

    lands = {1: from_left, -1: from_right}

    def reduce_send(d, step, u):
        send(("sum", d, step, u), part.at[at(z + d * (5 - step), u)], lands[d].at[2 * (step - 1) + u], z_dev(d))

    def reduce_add(d, step, u):
        slot = 2 * (step - 1) + u
        receive(("sum", d, step, u), lands[d].at[slot], z_dev(d))
        mine = at(z + d * (4 - step), u)
        part[mine] = part[mine] + lands[d][slot]

    def widen_queries(late):
        for d in (1, -1):
            ref, row = near_rows(d, late)
            receive(("q", d, late), ref, z_dev(d))
            widen(lambda at, row=row: near[pl.ds(row * HEADS + at, HEADS), :], row, QUARTER, as_feature)

    for d, u in ((1, 0), (-1, 1)):
        reduce_send(d, 1, u)
    for d, u in ((1, 1), (-1, 0)):
        reduce_send(d, 2, u)
    gather_1(0)
    for wave in (1, 2):
        send_own(wave)

    q_load.wait()
    widen(lambda row: k_in[pl.ds(row, HEADS), :], OWN, TOKENS, as_feature)
    widen_queries(False)

    for d, u in ((1, 0), (-1, 1)):
        reduce_add(d, 1, u)
        reduce_send(d, 2, u)
    gather_3(0, 0)
    for step in (2, 3):
        for u in (1, 0):
            for d in (1, -1):
                v = u if d == 1 else 1 - u
                reduce_add(d, step, v)
                reduce_send(d, step + 1, v)
        if step == 2:
            gather_2(0)
        else:
            gather_3(0, -1)

    def gather_send(d, step, u):
        ref = held.at[at(z - d * (step - 1), u)]
        send(("state", d, step, u), ref, ref, z_dev(d))

    def gather_take(d, step, u):
        receive(("state", d, step, u), held.at[at(z - d * step, u)], z_dev(d))

    def read_pair(i, blocks):
        terms = held[i, pl.ds(2 * SIZE, 32), :].astype(F32)
        block_at = i
        other_at = (i % RING) * RING + i // RING
        for u in (0, 1):
            head = 2 * i + u
            mass = terms[u : u + 1] + terms[8 + u : 9 + u] + terms[16 + u : 17 + u]
            state = held[i, pl.ds(u * SIZE, SIZE), :]
            for r, count in blocks:
                ask = wide[pl.ds(r * PITCH + head, count, stride=PITCH), :]
                bottom = jnp.sum(ask * mass, axis=1, keepdims=True) + 0.001
                top = jnp.dot(ask.astype(BF16), state, preferred_element_type=F32)
                result = (top * (2048.0**0.5 / bottom)).astype(BF16)
                for t, b in ((0, block_at), (1, other_at)):
                    to = pl.multiple_of(b * BLOCK + u * SIZE, SIZE)
                    mixed[t, pl.ds(r, count), pl.ds(to, SIZE)] = result

    EARLY = ((QUARTER, NEAR), (OWN, TOKENS))
    LATE = ((0, QUARTER), (3 * QUARTER, QUARTER))

    def read_pairs(first, count, blocks):
        def step(j, carry):
            read_pair(first + j, blocks)
            return carry

        lax.fori_loop(0, count, step, 0)

    def read_chunk(chunk):
        read_pairs(at(chunk, 0), 2, EARLY)

    mine = at(z, 0)
    for u in (0, 1):
        for d in (1, -1):
            receive(("sum", d, 4, u), lands[d].at[6 + u], z_dev(d))
        total = (part[mine + u] + from_left[6 + u] + from_right[6 + u]) * (1.0 / 2048.0)
        held[mine + u, pl.ds(0, 2 * SIZE), :] = total[: 2 * SIZE].astype(BF16)
        mass = total[2 * SIZE :]
        high = mass.astype(BF16).astype(F32)
        middle = (mass - high).astype(BF16).astype(F32)
        low = mass - high - middle
        terms = jnp.concatenate([high, middle, low, jnp.zeros_like(low)], axis=0)
        held[mine + u, pl.ds(2 * SIZE, 32), :] = terms.astype(BF16)
        for d in (1, -1):
            gather_send(d, 1, u)

    gather_3(0, 1)
    read_chunk(z)
    for step in (1, 2, 3):
        for u in (0, 1):
            for d in (1, -1):
                gather_take(d, step, u)
                if step < 3 or (u == 0) == (d == 1):
                    gather_send(d, step + 1, u)
        if step == 1:
            for wave in (1, 2):
                gather_1(wave)
        if step == 3:
            send_queries(True)
        for d in (1, -1):
            read_chunk(z - d * step)
    gather_take(1, 4, 0)
    gather_take(-1, 4, 1)
    read_chunk(z + 4)
    for wave in (1, 2):
        gather_3(wave, 0)
    gather_3(0, 2)
    widen_queries(True)
    read_pairs(0, PAIRS, LATE)

    def finish(wave):
        columns = pl.ds(pl.multiple_of(half * (WIDTH // 2) + STARTS[wave], 128), 2 * WAVES[wave])
        for d, row, to in ((-1, 0, NEAR), (1, NEAR, 0)):
            send(("out", wave, d), done[wave].at[pl.ds(row, NEAR), :], out.at[pl.ds(to, NEAR), columns], z_dev(d))

    def multiply(wave, rows_at, groups, first, last):
        tile = min(256, WAVES[wave])
        for t in (0, 1):

            def step(n, carry, t=t):
                column = pl.multiple_of(n * tile, tile)
                to = pl.multiple_of(t * WAVES[wave] + n * tile, tile)
                rows = pl.ds(rows_at, 256)
                total = None if first else accs[wave][rows, pl.ds(to, tile)]
                for dg in groups:
                    g = (g_at[t] + dg + RING) % RING
                    depth = pl.ds(pl.multiple_of(g * RING * BLOCK, RING * BLOCK), RING * BLOCK)
                    product = jnp.dot(
                        mixed[t, rows, depth], weights[wave][t, depth, pl.ds(column, tile)], preferred_element_type=F32
                    )
                    total = product if total is None else total + product
                if not last:
                    accs[wave][rows, pl.ds(to, tile)] = total
                elif rows_at == 0:
                    done[wave][:, pl.ds(to, tile)] = total.astype(BF16)
                else:
                    at = pl.multiple_of(half * (WIDTH // 2) + STARTS[wave] + to, 128)
                    out[:, pl.ds(at, tile)] = total.astype(BF16)
                return carry

            lax.fori_loop(0, WAVES[wave] // tile, step, 0)

    for rows_at in (0, OWN):
        multiply(0, rows_at, (0, -1, 1), True, False)
    for wave in (1, 2):
        gather_2(wave)
    gather_4(0)
    multiply(0, 0, (2,), False, True)
    finish(0)
    for wave in (1, 2):
        for j in (-1, 1):
            gather_3(wave, j)
    multiply(0, OWN, (2,), False, True)
    for wave in (1, 2):
        gather_3(wave, 2)
    for wave in (1, 2):
        for rows_at in (0, OWN):
            multiply(wave, rows_at, (0, -1, 1), True, False)
    for wave in (1, 2):
        gather_4(wave)
        multiply(wave, 0, (2,), False, True)
        finish(wave)
        multiply(wave, OWN, (2,), False, True)

    for copy in sent:
        copy.wait_send()
    for wave in range(len(WAVES)):
        columns = pl.ds(pl.multiple_of((1 - half) * (WIDTH // 2) + STARTS[wave], 128), 2 * WAVES[wave])
        for d, to in ((-1, NEAR), (1, 0)):
            receive(("out", wave, d), out.at[pl.ds(to, NEAR), columns], z_dev(d))
    assert len(ids) <= MESSAGES, len(ids)


MESSAGES = 158


def body(query_rows, key_rows, value_rows, out_weight):
    rows = [a.reshape(TOKENS * HEADS, SIZE) for a in (query_rows, key_rows, value_rows)]
    anywhere = pl.BlockSpec(memory_space=pltpu.HBM)
    result = pl.pallas_call(
        kernel,
        out_shape=pltpu.VMEM((TOKENS, WIDTH), BF16),
        in_specs=[anywhere] * 4,
        out_specs=pl.BlockSpec(memory_space=pltpu.VMEM),
        scratch_shapes=[pltpu.VMEM((2, WIDTH, columns), BF16) for columns in WAVES]
        + [pltpu.VMEM((ROWS, 2 * columns), F32) for columns in WAVES]
        + [pltpu.VMEM((OWN, 2 * columns), BF16) for columns in WAVES]
        + [
            pltpu.VMEM((TOKENS * HEADS, SIZE), BF16),
            pltpu.VMEM((TOKENS * HEADS, SIZE), BF16),
            pltpu.VMEM((OWN * HEADS, SIZE), BF16),
            pltpu.VMEM((ROWS * PITCH, SIZE), F32),
            pltpu.VMEM((PAIRS, SUMS, SIZE), F32),
            pltpu.VMEM((8, SUMS, SIZE), F32),
            pltpu.VMEM((8, SUMS, SIZE), F32),
            pltpu.VMEM((PAIRS, SENT, SIZE), BF16),
            pltpu.VMEM((2, ROWS, WIDTH), BF16),
            pltpu.SemaphoreType.DMA((2 * len(WAVES) + 3,)),
            pltpu.SemaphoreType.DMA((MESSAGES,)),
            pltpu.SemaphoreType.DMA((MESSAGES,)),
        ],
        compiler_params=pltpu.CompilerParams(
            collective_id=0, has_side_effects=True, vmem_limit_bytes=56 * 1024 * 1024
        ),
        name="attend",
    )(*rows, out_weight)
    return result.reshape(1, TOKENS, WIDTH)


def solution(mesh):
    placed = (
        P(("shift", "dp"), "sp", None, None),
        P(("shift", "dp"), "sp", None, None),
        P(("shift", "dp"), "sp", None, None),
        P(("shift", "dp"), None),
    )
    return jax.shard_map(
        body, mesh=mesh, in_specs=placed, out_specs=P(("shift", "dp"), "sp", None), check_vma=False
    )
```

```python
import jax
import jax.numpy as jnp
from jax import lax
from jax.experimental import pallas as pl
from jax.experimental.pallas import tpu as pltpu
from jax.sharding import PartitionSpec as P

MESH = pl.DeviceIdType.MESH
RING = 4
DEPTH = 8
HEADS = 32
SIZE = 128
TOKENS = 256
NEAR = 128
OWN = 2 * NEAR
ROWS = TOKENS + OWN
BLOCK = 256
WIDTH = 4096
PITCH = 40
WAVES = (512, 128, 128, 128, 128)
GIVE, TAKE = 1, 2
PAIRS = HEADS // 2
SUMS = 2 * SIZE + 8
SENT = 2 * SIZE + 32
F32 = jnp.float32
BF16 = jnp.bfloat16


def feature(values):
    return jnp.where(values > 0.0, values + 1.0, jnp.exp(jnp.minimum(values, 0.0)))


def kernel(q_hbm, k_hbm, v_hbm, w_hbm, out, *scratch):
    weights, scratch = scratch[: len(WAVES)], scratch[len(WAVES) :]
    acc, scratch = scratch[0], scratch[1:]
    done, scratch = scratch[: len(WAVES)], scratch[len(WAVES) :]
    k_in, v_in, near, wide, part, from_left, from_right, held, mixed, local_sem, send_sem, recv_sem = scratch
    dp = lax.axis_index("dp")
    z = lax.axis_index("sp")
    y, x = dp // RING, dp % RING
    half = z % 2

    def z_dev(step):
        return {"sp": (z + step + DEPTH) % DEPTH}

    def flat_dev(along, step):
        if along == "x":
            return {"dp": y * RING + (x + step + RING) % RING}
        return {"dp": ((y + step + RING) % RING) * RING + x}

    turn = (z // 2) % 2

    def columns_at(wave):
        start = 2 * sum(WAVES[:wave])
        if wave == GIVE:
            return start + 2 * WAVES[GIVE] * turn
        if wave == TAKE:
            return start - 2 * WAVES[GIVE] * turn
        return start

    send_ids, ids = {}, {}

    def copy_of(sent, key, src, dst, device):
        return pltpu.make_async_remote_copy(
            src_ref=src,
            dst_ref=dst,
            send_sem=send_sem.at[send_ids.setdefault(sent, len(send_ids))],
            recv_sem=recv_sem.at[ids.setdefault(key, len(ids))],
            device_id=device,
            device_id_type=MESH,
        )

    def send(sent, key, src, dst, device):
        copy_of(sent, key, src, dst, device).start()

    def receive(key, ref):
        copy_of(("own", 0), key, ref, ref, z_dev(1)).wait_recv()

    def all_sent(sent, ref):
        copy_of(sent, ("first", 0), ref, ref, z_dev(1)).wait_send()

    firsts, seconds = ("x", "y"), ("y", "x")
    f_at, g_at = (x, y), (y, x)

    def block(t, wave, df, dg, rows=None):
        f = (f_at[t] + df + RING) % RING
        g = (g_at[t] + dg + RING) % RING
        start = pl.multiple_of((g * RING + f) * BLOCK, BLOCK)
        if rows is None:
            return weights[wave].at[t, pl.ds(start, BLOCK), :]
        return weights[wave].at[t, pl.ds(pl.multiple_of(start + rows * (BLOCK // 2), BLOCK // 2), BLOCK // 2), :]

    def both(wave, blocks):
        return weights[wave].at[:, pl.ds(0, blocks * BLOCK), :]

    def pass_on(what, t, wave, ref, along, d):
        send(("own", wave), (what, wave), ref, ref, flat_dev(along[t], d))

    def send_second(t, wave, j):
        for d in (1, -1):
            pass_on(("second", j), t, wave, block(t, wave, j, 0), seconds, d)

    def gather_1(wave):
        receive(("first", wave), both(wave, 2))
        for t in (0, 1):
            for d in (1, -1):
                pass_on("first half", t, wave, block(t, wave, -d, 0, 0 if d == 1 else 1), firsts, d)
        for j in (-1, 1):
            for t in (0, 1):
                send_second(t, wave, j)

    def gather_2(wave):
        receive(("first half", wave), both(wave, 1))
        for t in (0, 1):
            send_second(t, wave, 2)

    def gather_3(wave, j):
        receive((("second", j), wave), both(wave, 2))
        if wave != TAKE:
            for t in (0, 1):
                for d in (1, -1):
                    pass_on("second half", t, wave, block(t, wave, j, -d, 0 if d == 1 else 1), seconds, d)

    def relay():
        for t in (0, 1):
            for d in (1, -1):
                g = (g_at[t] + 2) % RING
                rows = pl.ds(pl.multiple_of((g * RING + (0 if d == 1 else 2)) * BLOCK, BLOCK), 2 * BLOCK)
                send(
                    "relay",
                    ("second half", TAKE),
                    weights[GIVE].at[t, rows, :],
                    weights[TAKE].at[t, rows, :],
                    z_dev(2 * d),
                )

    def gather_4(wave):
        receive(("second half", wave), both(wave, 4))

    barrier = pltpu.get_barrier_semaphore()
    around = [flat_dev("x", 1), flat_dev("x", -1), flat_dev("y", 1), flat_dev("y", -1), z_dev(1), z_dev(-1)]
    around += [z_dev(2), z_dev(-2)]
    for device in around:
        pl.semaphore_signal(barrier, inc=1, device_id=device, device_id_type=MESH)
    loads = []
    for wave in range(len(WAVES)):
        for t in (0, 1):
            start = pl.multiple_of(half * (WIDTH // 2) + columns_at(wave) + t * WAVES[wave], 128)
            loads.append(
                pltpu.make_async_copy(
                    w_hbm.at[:, pl.ds(start, WAVES[wave])], block(t, wave, 0, 0), local_sem.at[wave]
                )
            )
    k_load = pltpu.make_async_copy(k_hbm, k_in, local_sem.at[len(WAVES)])
    v_load = pltpu.make_async_copy(v_hbm, v_in, local_sem.at[len(WAVES) + 1])
    q_load = pltpu.make_async_copy(q_hbm, k_in, local_sem.at[len(WAVES) + 2])
    for load in loads[:2] + [k_load, v_load] + loads[2:]:
        load.start()
    pl.semaphore_wait(barrier, len(around))

    def send_own(wave):
        ref = both(wave, 1)
        pltpu.make_async_copy(ref, ref, local_sem.at[wave]).wait()
        for t in (0, 1):
            for d in (1, -1):
                pass_on("first", t, wave, block(t, wave, 0, 0), firsts, d)
        for t in (0, 1):
            send_second(t, wave, 0)

    LOTS = ((0, 32), (32, 32), (64, 64))
    SOON = LOTS[0][1]

    def near_row(d, lot):
        start, count = LOTS[lot]
        return NEAR - start - count if d == 1 else NEAR + start

    def near_rows(d, lot):
        return near.at[pl.ds(near_row(d, lot) * HEADS, LOTS[lot][1] * HEADS), :]

    def send_queries(lot):
        for d in (1, -1):
            start, count = LOTS[lot]
            position = TOKENS - start - count if d == 1 else start
            send(
                "q",
                ("q", lot),
                q_hbm.at[pl.ds(position * HEADS, count * HEADS), :],
                near_rows(d, lot),
                z_dev(d),
            )

    send_own(0)
    send_own(GIVE)
    send_queries(0)

    def widen(src, at, count, fn):
        def step(i, carry):
            for u in range(4):
                row = pl.multiple_of((i * 4 + u) * HEADS, HEADS)
                to = pl.multiple_of((at + i * 4 + u) * PITCH, 8)
                wide[pl.ds(to, HEADS), :] = fn(src(row))
            return carry

        lax.fori_loop(0, count // 4, step, 0)

    def as_feature(values):
        return feature(values.astype(F32)).astype(BF16).astype(F32)

    k_load.wait()
    widen(lambda row: k_in[pl.ds(row, HEADS), :], 0, TOKENS, as_feature)
    q_load.start()
    v_load.wait()
    widen(lambda row: v_in[pl.ds(row, HEADS), :], TOKENS, TOKENS, lambda values: values.astype(F32))

    sub = lax.broadcasted_iota(jnp.int32, (8, SIZE), 0)

    def states(i, carry):
        masses = []
        for u in (0, 1):
            head = 2 * i + u
            keys = wide[pl.ds(head, TOKENS, stride=PITCH), :]
            values = wide[pl.ds(TOKENS * PITCH + head, TOKENS, stride=PITCH), :]
            part[i, pl.ds(u * SIZE, SIZE), :] = lax.dot_general(
                keys.astype(BF16), values.astype(BF16), (((0,), (0,)), ((), ())), preferred_element_type=F32
            )
            masses.append(jnp.sum(keys, axis=0, keepdims=True))
        part[i, pl.ds(2 * SIZE, 8), :] = jnp.where(sub == 0, masses[0], jnp.where(sub == 1, masses[1], 0.0))
        return carry

    lax.fori_loop(0, PAIRS, states, 0)

    def at(chunk, u):
        return ((chunk + 2 * DEPTH) % DEPTH) * 2 + u

    lands = {1: from_left, -1: from_right}

    def reduce_send(d, step, u):
        send("sum", ("sum", d, step, u), part.at[at(z + d * (5 - step), u)], lands[d].at[2 * (step - 1) + u], z_dev(d))

    def reduce_add(d, step, u):
        slot = 2 * (step - 1) + u
        receive(("sum", d, step, u), lands[d].at[slot])
        mine = at(z + d * (4 - step), u)
        part[mine] = part[mine] + lands[d][slot]

    def widen_queries(lot):
        receive(("q", lot), near.at[pl.ds(0, 2 * LOTS[lot][1] * HEADS), :])
        for d in (1, -1):
            row = near_row(d, lot)
            widen(lambda at, row=row: near[pl.ds(row * HEADS + at, HEADS), :], row, LOTS[lot][1], as_feature)

    for d, u in ((1, 0), (-1, 1)):
        reduce_send(d, 1, u)
    for d, u in ((1, 1), (-1, 0)):
        reduce_send(d, 2, u)
    gather_1(0)

    q_load.wait()
    widen(lambda row: k_in[pl.ds(row, HEADS), :], OWN, TOKENS, as_feature)
    widen_queries(0)

    for d, u in ((1, 0), (-1, 1)):
        reduce_add(d, 1, u)
        reduce_send(d, 2, u)
    gather_3(0, 0)
    for step in (2, 3):
        for u in (1, 0):
            for d in (1, -1):
                v = u if d == 1 else 1 - u
                reduce_add(d, step, v)
                reduce_send(d, step + 1, v)
        if step == 2:
            gather_2(0)
            gather_1(1)
        else:
            send_queries(1)
            gather_3(0, -1)
            gather_3(1, 0)

    def gather_send(d, step, u):
        ref = held.at[at(z - d * (step - 1), u)]
        send("state", ("state", d, step, u), ref, ref, z_dev(d))

    def gather_take(d, step, u):
        receive(("state", d, step, u), held.at[at(z - d * step, u)])

    def read_pair(i, blocks):
        terms = held[i, pl.ds(2 * SIZE, 32), :].astype(F32)
        block_at = i
        other_at = (i % RING) * RING + i // RING
        for u in (0, 1):
            head = 2 * i + u
            mass = terms[u : u + 1] + terms[8 + u : 9 + u] + terms[16 + u : 17 + u]
            state = held[i, pl.ds(u * SIZE, SIZE), :]
            for r, count in blocks:
                ask = wide[pl.ds(r * PITCH + head, count, stride=PITCH), :]
                bottom = jnp.sum(ask * mass, axis=1, keepdims=True) + 0.001
                top = jnp.dot(ask.astype(BF16), state, preferred_element_type=F32)
                result = (top * (2048.0**0.5 / bottom)).astype(BF16)
                for t, b in ((0, block_at), (1, other_at)):
                    to = pl.multiple_of(b * BLOCK + u * SIZE, SIZE)
                    mixed[t, pl.ds(r, count), pl.ds(to, SIZE)] = result

    EARLY = ((NEAR - SOON, 2 * SOON), (OWN, TOKENS))
    LATE = ((0, NEAR - SOON), (NEAR + SOON, NEAR - SOON))

    def read_pairs(first, count, blocks):
        def step(j, carry):
            read_pair(first + j, blocks)
            return carry

        lax.fori_loop(0, count, step, 0)

    def read_chunk(chunk):
        read_pairs(at(chunk, 0), 2, EARLY)

    mine = at(z, 0)
    for u in (0, 1):
        for d in (1, -1):
            receive(("sum", d, 4, u), lands[d].at[6 + u])
        total = (part[mine + u] + from_left[6 + u] + from_right[6 + u]) * (1.0 / 2048.0)
        held[mine + u, pl.ds(0, 2 * SIZE), :] = total[: 2 * SIZE].astype(BF16)
        mass = total[2 * SIZE :]
        high = mass.astype(BF16).astype(F32)
        middle = (mass - high).astype(BF16).astype(F32)
        low = mass - high - middle
        terms = jnp.concatenate([high, middle, low, jnp.zeros_like(low)], axis=0)
        held[mine + u, pl.ds(2 * SIZE, 32), :] = terms.astype(BF16)
        for d in (1, -1):
            gather_send(d, 1, u)

    read_chunk(z)
    gather_3(0, 1)
    for step in (1, 2, 3):
        for u in (0, 1):
            for d in (1, -1):
                gather_take(d, step, u)
                if step < 3 or (u == 0) == (d == 1):
                    gather_send(d, step + 1, u)
        if step == 2:
            gather_2(1)
            gather_3(0, 2)
            send_own(2)
        if step == 3:
            send_queries(2)
            gather_3(1, -1)
            gather_3(1, 1)
        for d in (1, -1):
            read_chunk(z - d * step)
    gather_take(1, 4, 0)
    gather_take(-1, 4, 1)
    read_chunk(z + 4)

    def finish(wave):
        columns = pl.ds(pl.multiple_of(half * (WIDTH // 2) + columns_at(wave), 128), 2 * WAVES[wave])
        for d, row, to in ((-1, 0, NEAR), (1, NEAR, 0)):
            send(
                ("out", wave),
                ("out", wave),
                done[wave].at[pl.ds(row, NEAR), :],
                out.at[pl.ds(to, NEAR), columns],
                z_dev(d),
            )

    def multiply(wave, rows_at, groups, first, last):
        tile = 256 if WAVES[wave] % 256 == 0 else 128
        for t in (0, 1):

            def step(n, carry, t=t):
                column = pl.multiple_of(n * tile, tile)
                to = pl.multiple_of(t * WAVES[wave] + n * tile, tile)
                rows = pl.ds(rows_at, 256)
                total = None if first else acc[rows, pl.ds(to, tile)]
                for dg in groups:
                    g = (g_at[t] + dg + RING) % RING
                    depth = pl.ds(pl.multiple_of(g * RING * BLOCK, RING * BLOCK), RING * BLOCK)
                    product = jnp.dot(
                        mixed[t, rows, depth], weights[wave][t, depth, pl.ds(column, tile)], preferred_element_type=F32
                    )
                    total = product if total is None else total + product
                if not last:
                    acc[rows, pl.ds(to, tile)] = total
                elif rows_at == 0:
                    done[wave][:, pl.ds(to, tile)] = total.astype(BF16)
                else:
                    at = pl.multiple_of(half * (WIDTH // 2) + columns_at(wave) + to, 128)
                    out[:, pl.ds(at, tile)] = total.astype(BF16)
                return carry

            lax.fori_loop(0, WAVES[wave] // tile, step, 0)

    WHOLE = (0, -1, 1, 2)

    def near_products(wave):
        multiply(wave, 0, WHOLE, True, True)
        finish(wave)

    def own_products(wave):
        multiply(wave, OWN, WHOLE, True, True)

    send_own(3)
    gather_3(1, 2)
    gather_4(0)
    own_products(0)
    gather_1(2)
    gather_4(1)
    relay()
    send_own(4)
    widen_queries(1)
    widen_queries(2)
    read_pairs(0, PAIRS, LATE)
    gather_3(2, 0)
    gather_1(3)
    gather_2(2)
    near_products(0)
    gather_3(3, 0)
    gather_2(3)
    gather_1(4)
    near_products(1)
    gather_3(2, -1)
    gather_3(2, 1)
    gather_3(3, -1)
    gather_3(3, 1)
    own_products(1)
    gather_3(3, 2)
    gather_3(4, 0)
    gather_2(4)
    gather_3(2, 2)
    gather_4(2)
    near_products(2)
    gather_3(4, -1)
    gather_3(4, 1)
    own_products(2)
    gather_4(3)
    near_products(3)
    gather_3(4, 2)
    own_products(3)
    for rows_at in (0, OWN):
        multiply(4, rows_at, (0, -1, 1), True, False)
    gather_4(4)
    multiply(4, 0, (2,), False, True)
    finish(4)
    multiply(4, OWN, (2,), False, True)

    for wave in range(len(WAVES)):
        all_sent(("own", wave), both(wave, 11 if wave == TAKE else 15))
    all_sent("relay", both(GIVE, 4))
    all_sent("q", near)
    all_sent("sum", part.at[pl.ds(0, 14)])
    all_sent("state", held.at[pl.ds(0, 14)])
    for wave in range(len(WAVES)):
        all_sent(("out", wave), done[wave])
    for wave in range(len(WAVES)):
        receive(("out", wave), done[wave])
    assert len(send_ids) <= SENDS and len(ids) <= RECEIVES, (len(send_ids), len(ids))


SENDS = 14
RECEIVES = 72


def body(query_rows, key_rows, value_rows, out_weight):
    rows = [a.reshape(TOKENS * HEADS, SIZE) for a in (query_rows, key_rows, value_rows)]
    anywhere = pl.BlockSpec(memory_space=pltpu.HBM)
    result = pl.pallas_call(
        kernel,
        out_shape=pltpu.VMEM((TOKENS, WIDTH), BF16),
        in_specs=[anywhere] * 4,
        out_specs=pl.BlockSpec(memory_space=pltpu.VMEM),
        scratch_shapes=[pltpu.VMEM((2, WIDTH, columns), BF16) for columns in WAVES]
        + [pltpu.VMEM((ROWS, 2 * columns), F32) for columns in WAVES[-1:]]
        + [pltpu.VMEM((OWN, 2 * columns), BF16) for columns in WAVES]
        + [
            pltpu.VMEM((TOKENS * HEADS, SIZE), BF16),
            pltpu.VMEM((TOKENS * HEADS, SIZE), BF16),
            pltpu.VMEM((OWN * HEADS, SIZE), BF16),
            pltpu.VMEM((ROWS * PITCH, SIZE), F32),
            pltpu.VMEM((PAIRS, SUMS, SIZE), F32),
            pltpu.VMEM((8, SUMS, SIZE), F32),
            pltpu.VMEM((8, SUMS, SIZE), F32),
            pltpu.VMEM((PAIRS, SENT, SIZE), BF16),
            pltpu.VMEM((2, ROWS, WIDTH), BF16),
            pltpu.SemaphoreType.DMA((len(WAVES) + 3,)),
            pltpu.SemaphoreType.DMA((SENDS,)),
            pltpu.SemaphoreType.DMA((RECEIVES,)),
        ],
        compiler_params=pltpu.CompilerParams(
            collective_id=0, has_side_effects=True, vmem_limit_bytes=56 * 1024 * 1024
        ),
        name="attend",
    )(*rows, out_weight)
    return result.reshape(1, TOKENS, WIDTH)


def solution(mesh):
    placed = (
        P(("shift", "dp"), "sp", None, None),
        P(("shift", "dp"), "sp", None, None),
        P(("shift", "dp"), "sp", None, None),
        P(("shift", "dp"), None),
    )
    return jax.shard_map(
        body, mesh=mesh, in_specs=placed, out_specs=P(("shift", "dp"), "sp", None), check_vma=False
    )
```

```python
import functools

import jax
import jax.numpy as jnp
from jax import lax
from jax.experimental import pallas as pl
from jax.experimental.pallas import tpu as pltpu
from jax.sharding import PartitionSpec as P

MESH = pl.DeviceIdType.MESH
RING = 4
DEPTH = 8
HEADS = 32
SIZE = 128
TOKENS = 256
NEAR = 128
OWN = 2 * NEAR
ROWS = TOKENS + OWN
BLOCK = 256
WIDTH = 4096
PITCH = 40
WAVES = (512, 128, 128, 128, 128)
GIVE, TAKE = 1, 2
PAIRS = HEADS // 2
SUMS = 2 * SIZE + 8
SENT = 2 * SIZE + 32
F32 = jnp.float32
BF16 = jnp.bfloat16


def feature(values):
    return jnp.where(values > 0.0, values + 1.0, jnp.exp(jnp.minimum(values, 0.0)))


def kernel(q_hbm, k_hbm, v_hbm, w_hbm, out, *scratch):
    weights, scratch = scratch[: len(WAVES)], scratch[len(WAVES) :]
    acc, scratch = scratch[0], scratch[1:]
    done, scratch = scratch[: len(WAVES)], scratch[len(WAVES) :]
    k_in, v_in, near, wide, part, from_left, from_right, held, mixed, local_sem, send_sem, recv_sem = scratch
    dp = lax.axis_index("dp")
    z = lax.axis_index("sp")
    y, x = dp // RING, dp % RING
    half = z % 2

    def z_dev(step):
        return {"sp": (z + step + DEPTH) % DEPTH}

    def flat_dev(along, step):
        if along == "x":
            return {"dp": y * RING + (x + step + RING) % RING}
        return {"dp": ((y + step + RING) % RING) * RING + x}

    turn = (z // 2) % 2

    def columns_at(wave):
        start = 2 * sum(WAVES[:wave])
        if wave == GIVE:
            return start + 2 * WAVES[GIVE] * turn
        if wave == TAKE:
            return start - 2 * WAVES[GIVE] * turn
        return start

    send_ids, ids = {}, {}

    def copy_of(sent, key, src, dst, device):
        return pltpu.make_async_remote_copy(
            src_ref=src,
            dst_ref=dst,
            send_sem=send_sem.at[send_ids.setdefault(sent, len(send_ids))],
            recv_sem=recv_sem.at[ids.setdefault(key, len(ids))],
            device_id=device,
            device_id_type=MESH,
        )

    def send(sent, key, src, dst, device):
        copy_of(sent, key, src, dst, device).start()

    def receive(key, ref):
        copy_of(("own", 0), key, ref, ref, z_dev(1)).wait_recv()

    def all_sent(sent, ref):
        copy_of(sent, ("first", 0), ref, ref, z_dev(1)).wait_send()

    firsts, seconds = ("x", "y"), ("y", "x")
    f_at, g_at = (x, y), (y, x)

    def block(t, wave, df, dg, rows=None):
        f = (f_at[t] + df + RING) % RING
        g = (g_at[t] + dg + RING) % RING
        start = pl.multiple_of((g * RING + f) * BLOCK, BLOCK)
        if rows is None:
            return weights[wave].at[t, pl.ds(start, BLOCK), :]
        return weights[wave].at[t, pl.ds(pl.multiple_of(start + rows * (BLOCK // 2), BLOCK // 2), BLOCK // 2), :]

    def both(wave, blocks):
        return weights[wave].at[:, pl.ds(0, blocks * BLOCK), :]

    def pass_on(what, t, wave, ref, along, d):
        send(("own", wave), (what, wave), ref, ref, flat_dev(along[t], d))

    def send_second(t, wave, j):
        for d in (1, -1):
            pass_on(("second", j), t, wave, block(t, wave, j, 0), seconds, d)

    def gather_1(wave):
        receive(("first", wave), both(wave, 2))
        for t in (0, 1):
            for d in (1, -1):
                pass_on("first half", t, wave, block(t, wave, -d, 0, 0 if d == 1 else 1), firsts, d)
        for j in (-1, 1):
            for t in (0, 1):
                send_second(t, wave, j)

    def gather_2(wave):
        receive(("first half", wave), both(wave, 1))
        for t in (0, 1):
            send_second(t, wave, 2)

    def gather_3(wave, j):
        receive((("second", j), wave), both(wave, 2))
        if wave != TAKE:
            for t in (0, 1):
                for d in (1, -1):
                    pass_on("second half", t, wave, block(t, wave, j, -d, 0 if d == 1 else 1), seconds, d)

    def relay():
        for t in (0, 1):
            for d in (1, -1):
                g = (g_at[t] + 2) % RING
                rows = pl.ds(pl.multiple_of((g * RING + (0 if d == 1 else 2)) * BLOCK, BLOCK), 2 * BLOCK)
                send(
                    "relay",
                    ("second half", TAKE),
                    weights[GIVE].at[t, rows, :],
                    weights[TAKE].at[t, rows, :],
                    z_dev(2 * d),
                )

    def gather_4(wave):
        receive(("second half", wave), both(wave, 4))

    barrier = pltpu.get_barrier_semaphore()
    around = [flat_dev("x", 1), flat_dev("x", -1), flat_dev("y", 1), flat_dev("y", -1), z_dev(1), z_dev(-1)]
    around += [z_dev(2), z_dev(-2)]
    for device in around:
        pl.semaphore_signal(barrier, inc=1, device_id=device, device_id_type=MESH)
    loads = []
    for wave in range(len(WAVES)):
        for t in (0, 1):
            start = pl.multiple_of(half * (WIDTH // 2) + columns_at(wave) + t * WAVES[wave], 128)
            loads.append(
                pltpu.make_async_copy(
                    w_hbm.at[:, pl.ds(start, WAVES[wave])], block(t, wave, 0, 0), local_sem.at[wave]
                )
            )
    k_load = pltpu.make_async_copy(k_hbm, k_in, local_sem.at[len(WAVES)])
    v_load = pltpu.make_async_copy(v_hbm, v_in, local_sem.at[len(WAVES) + 1])
    q_load = pltpu.make_async_copy(q_hbm, k_in, local_sem.at[len(WAVES) + 2])
    for load in loads[:2] + [k_load, v_load] + loads[2:]:
        load.start()
    pl.semaphore_wait(barrier, len(around))

    def send_own(wave):
        ref = both(wave, 1)
        pltpu.make_async_copy(ref, ref, local_sem.at[wave]).wait()
        for t in (0, 1):
            for d in (1, -1):
                pass_on("first", t, wave, block(t, wave, 0, 0), firsts, d)
        for t in (0, 1):
            send_second(t, wave, 0)

    LOTS = ((0, 32), (32, 32), (64, 64))
    SOON = LOTS[0][1]

    def near_row(d, lot):
        start, count = LOTS[lot]
        return NEAR - start - count if d == 1 else NEAR + start

    def near_rows(d, lot):
        return near.at[pl.ds(near_row(d, lot) * HEADS, LOTS[lot][1] * HEADS), :]

    def send_queries(lot):
        for d in (1, -1):
            start, count = LOTS[lot]
            position = TOKENS - start - count if d == 1 else start
            send(
                "q",
                ("q", lot),
                q_hbm.at[pl.ds(position * HEADS, count * HEADS), :],
                near_rows(d, lot),
                z_dev(d),
            )

    send_own(0)
    send_own(GIVE)
    send_queries(0)

    def widen(src, at, count, fn):
        def step(i, carry):
            for u in range(4):
                row = pl.multiple_of((i * 4 + u) * HEADS, HEADS)
                to = pl.multiple_of((at + i * 4 + u) * PITCH, 8)
                wide[pl.ds(to, HEADS), :] = fn(src(row))
            return carry

        lax.fori_loop(0, count // 4, step, 0)

    def as_feature(values):
        return feature(values.astype(F32)).astype(BF16).astype(F32)

    k_load.wait()
    widen(lambda row: k_in[pl.ds(row, HEADS), :], 0, TOKENS, as_feature)
    q_load.start()
    v_load.wait()
    widen(lambda row: v_in[pl.ds(row, HEADS), :], TOKENS, TOKENS, lambda values: values.astype(F32))

    sub = lax.broadcasted_iota(jnp.int32, (8, SIZE), 0)

    def states(i, carry):
        masses = []
        for u in (0, 1):
            head = 2 * i + u
            keys = wide[pl.ds(head, TOKENS, stride=PITCH), :]
            values = wide[pl.ds(TOKENS * PITCH + head, TOKENS, stride=PITCH), :]
            part[i, pl.ds(u * SIZE, SIZE), :] = lax.dot_general(
                keys.astype(BF16), values.astype(BF16), (((0,), (0,)), ((), ())), preferred_element_type=F32
            )
            masses.append(jnp.sum(keys, axis=0, keepdims=True))
        part[i, pl.ds(2 * SIZE, 8), :] = jnp.where(sub == 0, masses[0], jnp.where(sub == 1, masses[1], 0.0))
        return carry

    lax.fori_loop(0, PAIRS, states, 0)

    def at(chunk, u):
        return ((chunk + 2 * DEPTH) % DEPTH) * 2 + u

    lands = {1: from_left, -1: from_right}

    def reduce_send(d, step, u):
        send("sum", ("sum", d, step, u), part.at[at(z + d * (5 - step), u)], lands[d].at[2 * (step - 1) + u], z_dev(d))

    def reduce_add(d, step, u):
        slot = 2 * (step - 1) + u
        receive(("sum", d, step, u), lands[d].at[slot])
        mine = at(z + d * (4 - step), u)
        part[mine] = part[mine] + lands[d][slot]

    def widen_queries(lot):
        receive(("q", lot), near.at[pl.ds(0, 2 * LOTS[lot][1] * HEADS), :])
        for d in (1, -1):
            row = near_row(d, lot)
            widen(lambda at, row=row: near[pl.ds(row * HEADS + at, HEADS), :], row, LOTS[lot][1], as_feature)

    for d, u in ((1, 0), (-1, 1)):
        reduce_send(d, 1, u)
    for d, u in ((1, 1), (-1, 0)):
        reduce_send(d, 2, u)
    gather_1(0)

    q_load.wait()
    widen(lambda row: k_in[pl.ds(row, HEADS), :], OWN, TOKENS, as_feature)
    widen_queries(0)

    def reduce_step(step, u):
        for d in (1, -1):
            v = u if d == 1 else 1 - u
            reduce_add(d, step, v)
            reduce_send(d, step + 1, v)

    def gather_send(d, step, u):
        ref = held.at[at(z - d * (step - 1), u)]
        send("state", ("state", d, step, u), ref, ref, z_dev(d))

    def gather_take(d, step, u):
        receive(("state", d, step, u), held.at[at(z - d * step, u)])

    def read_pair(i, blocks):
        terms = held[i, pl.ds(2 * SIZE, 32), :].astype(F32)
        block_at = i
        other_at = (i % RING) * RING + i // RING
        for u in (0, 1):
            head = 2 * i + u
            mass = terms[u : u + 1] + terms[8 + u : 9 + u] + terms[16 + u : 17 + u]
            state = held[i, pl.ds(u * SIZE, SIZE), :]
            for r, count in blocks:
                ask = wide[pl.ds(r * PITCH + head, count, stride=PITCH), :]
                bottom = jnp.sum(ask * mass, axis=1, keepdims=True) + 0.001
                top = jnp.dot(ask.astype(BF16), state, preferred_element_type=F32)
                result = (top * (2048.0**0.5 / bottom)).astype(BF16)
                for t, b in ((0, block_at), (1, other_at)):
                    to = pl.multiple_of(b * BLOCK + u * SIZE, SIZE)
                    mixed[t, pl.ds(r, count), pl.ds(to, SIZE)] = result

    EARLY = ((NEAR - SOON, 2 * SOON), (OWN, TOKENS))
    LATE = ((0, NEAR - SOON), (NEAR + SOON, NEAR - SOON))

    def read_pairs(first, count, blocks):
        def step(j, carry):
            read_pair(first + j, blocks)
            return carry

        lax.fori_loop(0, count, step, 0)

    def read_chunk(chunk):
        read_pairs(at(chunk, 0), 2, EARLY)

    def own_sums():
        mine = at(z, 0)
        for u in (0, 1):
            for d in (1, -1):
                receive(("sum", d, 4, u), lands[d].at[6 + u])
            total = (part[mine + u] + from_left[6 + u] + from_right[6 + u]) * (1.0 / 2048.0)
            held[mine + u, pl.ds(0, 2 * SIZE), :] = total[: 2 * SIZE].astype(BF16)
            mass = total[2 * SIZE :]
            high = mass.astype(BF16).astype(F32)
            middle = (mass - high).astype(BF16).astype(F32)
            low = mass - high - middle
            terms = jnp.concatenate([high, middle, low, jnp.zeros_like(low)], axis=0)
            held[mine + u, pl.ds(2 * SIZE, 32), :] = terms.astype(BF16)
            for d in (1, -1):
                gather_send(d, 1, u)

    def gather_step(step):
        for u in (0, 1):
            for d in (1, -1):
                if step < 4 or (u == 0) == (d == 1):
                    gather_take(d, step, u)
                    if step < 3 or (step == 3 and (u == 0) == (d == 1)):
                        gather_send(d, step + 1, u)

    def read_step(step):
        for d in (1, -1) if step < 4 else (1,):
            read_chunk(z - d * step)

    def finish(wave):
        columns = pl.ds(pl.multiple_of(half * (WIDTH // 2) + columns_at(wave), 128), 2 * WAVES[wave])
        for d, row, to in ((-1, 0, NEAR), (1, NEAR, 0)):
            send(
                ("out", wave),
                ("out", wave),
                done[wave].at[pl.ds(row, NEAR), :],
                out.at[pl.ds(to, NEAR), columns],
                z_dev(d),
            )

    def multiply(wave, rows_at, groups, first, last):
        for t in (0, 1):

            def step(start, tile, n, carry, t=t):
                column = pl.multiple_of(start + n * tile, tile)
                to = pl.multiple_of(t * WAVES[wave] + start + n * tile, 128)
                rows = pl.ds(rows_at, 256)
                total = None if first else acc[rows, pl.ds(to, tile)]
                for dg in groups:
                    g = (g_at[t] + dg + RING) % RING
                    depth = pl.ds(pl.multiple_of(g * RING * BLOCK, RING * BLOCK), RING * BLOCK)
                    product = jnp.dot(
                        mixed[t, rows, depth], weights[wave][t, depth, pl.ds(column, tile)], preferred_element_type=F32
                    )
                    total = product if total is None else total + product
                if not last:
                    acc[rows, pl.ds(to, tile)] = total
                elif rows_at == 0:
                    done[wave][:, pl.ds(to, tile)] = total.astype(BF16)
                else:
                    at = pl.multiple_of(half * (WIDTH // 2) + columns_at(wave) + to, 128)
                    out[:, pl.ds(at, tile)] = total.astype(BF16)
                return carry

            pairs, rest = divmod(WAVES[wave], 256)
            if pairs:
                lax.fori_loop(0, pairs, functools.partial(step, 0, 256), 0)
            if rest:
                step(pairs * 256, rest, 0, 0)

    WHOLE = (0, -1, 1, 2)

    def near_products(wave):
        multiply(wave, 0, WHOLE, True, True)
        finish(wave)

    def own_products(wave):
        multiply(wave, OWN, WHOLE, True, True)

    gather_3(0, 0)
    for d, u in ((1, 0), (-1, 1)):
        reduce_add(d, 1, u)
        reduce_send(d, 2, u)
    gather_1(1)
    reduce_step(2, 1)
    reduce_step(2, 0)
    send_own(3)
    reduce_step(3, 1)
    reduce_step(3, 0)
    send_queries(2)
    own_sums()
    gather_2(1)
    gather_3(1, 0)
    gather_1(3)
    gather_2(0)
    gather_3(1, 2)
    gather_3(1, -1)
    send_own(2)
    read_chunk(z)
    gather_step(1)
    gather_3(1, 1)
    send_queries(1)
    gather_step(2)
    gather_3(0, 1)
    gather_1(2)
    gather_step(3)
    read_step(1)
    gather_2(3)
    gather_3(0, -1)
    gather_3(0, 2)
    read_step(2)
    widen_queries(1)
    widen_queries(2)
    gather_4(1)
    gather_3(3, -1)
    read_step(3)
    relay()
    gather_step(4)
    gather_3(3, 1)
    send_own(4)
    read_step(4)
    own_products(1)
    read_pairs(0, PAIRS, LATE)
    near_products(1)
    gather_3(2, 1)
    gather_3(3, 0)
    gather_3(3, 2)
    gather_4(0)
    own_products(0)
    gather_1(4)
    near_products(0)
    gather_2(4)
    gather_4(3)
    gather_3(2, -1)
    gather_2(2)
    gather_3(4, 0)
    gather_3(2, 0)
    gather_3(4, -1)
    near_products(3)
    own_products(3)
    gather_3(4, 1)
    gather_3(4, 2)
    multiply(4, 0, (0, -1, 1), True, False)
    gather_4(2)
    gather_3(2, 2)
    near_products(2)
    own_products(2)
    gather_4(4)
    multiply(4, 0, (2,), False, True)
    finish(4)
    multiply(4, OWN, (0, -1, 1), True, False)
    multiply(4, OWN, (2,), False, True)

    for wave in range(len(WAVES)):
        all_sent(("own", wave), both(wave, 11 if wave == TAKE else 15))
    all_sent("relay", both(GIVE, 4))
    all_sent("q", near)
    all_sent("sum", part.at[pl.ds(0, 14)])
    all_sent("state", held.at[pl.ds(0, 14)])
    for wave in range(len(WAVES)):
        all_sent(("out", wave), done[wave])
    for wave in range(len(WAVES)):
        receive(("out", wave), done[wave])
    assert len(send_ids) <= SENDS and len(ids) <= RECEIVES, (len(send_ids), len(ids))


SENDS = 14
RECEIVES = 72


def body(query_rows, key_rows, value_rows, out_weight):
    rows = [a.reshape(TOKENS * HEADS, SIZE) for a in (query_rows, key_rows, value_rows)]
    anywhere = pl.BlockSpec(memory_space=pltpu.HBM)
    result = pl.pallas_call(
        kernel,
        out_shape=pltpu.VMEM((TOKENS, WIDTH), BF16),
        in_specs=[anywhere] * 4,
        out_specs=pl.BlockSpec(memory_space=pltpu.VMEM),
        scratch_shapes=[pltpu.VMEM((2, WIDTH, columns), BF16) for columns in WAVES]
        + [pltpu.VMEM((ROWS, 2 * columns), F32) for columns in WAVES[-1:]]
        + [pltpu.VMEM((OWN, 2 * columns), BF16) for columns in WAVES]
        + [
            pltpu.VMEM((TOKENS * HEADS, SIZE), BF16),
            pltpu.VMEM((TOKENS * HEADS, SIZE), BF16),
            pltpu.VMEM((OWN * HEADS, SIZE), BF16),
            pltpu.VMEM((ROWS * PITCH, SIZE), F32),
            pltpu.VMEM((PAIRS, SUMS, SIZE), F32),
            pltpu.VMEM((8, SUMS, SIZE), F32),
            pltpu.VMEM((8, SUMS, SIZE), F32),
            pltpu.VMEM((PAIRS, SENT, SIZE), BF16),
            pltpu.VMEM((2, ROWS, WIDTH), BF16),
            pltpu.SemaphoreType.DMA((len(WAVES) + 3,)),
            pltpu.SemaphoreType.DMA((SENDS,)),
            pltpu.SemaphoreType.DMA((RECEIVES,)),
        ],
        compiler_params=pltpu.CompilerParams(
            collective_id=0, has_side_effects=True, vmem_limit_bytes=56 * 1024 * 1024
        ),
        name="attend",
    )(*rows, out_weight)
    return result.reshape(1, TOKENS, WIDTH)


def solution(mesh):
    placed = (
        P(("shift", "dp"), "sp", None, None),
        P(("shift", "dp"), "sp", None, None),
        P(("shift", "dp"), "sp", None, None),
        P(("shift", "dp"), None),
    )
    return jax.shard_map(
        body, mesh=mesh, in_specs=placed, out_specs=P(("shift", "dp"), "sp", None), check_vma=False
    )
```

```python
import functools

import jax
import jax.numpy as jnp
from jax import lax
from jax.experimental import pallas as pl
from jax.experimental.pallas import tpu as pltpu
from jax.sharding import PartitionSpec as P

MESH = pl.DeviceIdType.MESH
RING = 4
DEPTH = 8
HEADS = 32
SIZE = 128
TOKENS = 256
NEAR = 128
OWN = 2 * NEAR
ROWS = TOKENS + OWN
BLOCK = 256
WIDTH = 4096
PITCH = 40
WAVES = (512, 128, 128, 128, 128)
GIVE, TAKE = 1, 2
PAIRS = HEADS // 2
SUMS = 2 * SIZE + 8
SENT = 2 * SIZE + 16
F32 = jnp.float32
BF16 = jnp.bfloat16


def feature(values):
    return jnp.where(values > 0.0, values + 1.0, jnp.exp(jnp.minimum(values, 0.0)))


def kernel(q_hbm, k_hbm, v_hbm, w_hbm, out, *scratch):
    weights, scratch = scratch[: len(WAVES)], scratch[len(WAVES) :]
    acc, scratch = scratch[0], scratch[1:]
    done, scratch = scratch[: len(WAVES)], scratch[len(WAVES) :]
    k_in, v_in, near, wide, part, from_left, from_right, held, mixed, local_sem, send_sem, recv_sem = scratch
    dp = lax.axis_index("dp")
    z = lax.axis_index("sp")
    y, x = dp // RING, dp % RING
    half = z % 2

    def z_dev(step):
        return {"sp": (z + step + DEPTH) % DEPTH}

    def flat_dev(along, step):
        if along == "x":
            return {"dp": y * RING + (x + step + RING) % RING}
        return {"dp": ((y + step + RING) % RING) * RING + x}

    turn = (z // 2) % 2

    def columns_at(wave):
        start = 2 * sum(WAVES[:wave])
        if wave == GIVE:
            return start + 2 * WAVES[GIVE] * turn
        if wave == TAKE:
            return start - 2 * WAVES[GIVE] * turn
        return start

    send_ids, ids = {}, {}

    def copy_of(sent, key, src, dst, device):
        return pltpu.make_async_remote_copy(
            src_ref=src,
            dst_ref=dst,
            send_sem=send_sem.at[send_ids.setdefault(sent, len(send_ids))],
            recv_sem=recv_sem.at[ids.setdefault(key, len(ids))],
            device_id=device,
            device_id_type=MESH,
        )

    def send(sent, key, src, dst, device):
        copy_of(sent, key, src, dst, device).start()

    def receive(key, ref):
        copy_of(("own", 0), key, ref, ref, z_dev(1)).wait_recv()

    def all_sent(sent, ref):
        copy_of(sent, ("first", 0), ref, ref, z_dev(1)).wait_send()

    firsts, seconds = ("x", "y"), ("y", "x")
    f_at, g_at = (x, y), (y, x)

    def block(t, wave, df, dg, rows=None):
        f = (f_at[t] + df + RING) % RING
        g = (g_at[t] + dg + RING) % RING
        start = pl.multiple_of((g * RING + f) * BLOCK, BLOCK)
        if rows is None:
            return weights[wave].at[t, pl.ds(start, BLOCK), :]
        return weights[wave].at[t, pl.ds(pl.multiple_of(start + rows * (BLOCK // 2), BLOCK // 2), BLOCK // 2), :]

    def both(wave, blocks):
        return weights[wave].at[:, pl.ds(0, blocks * BLOCK), :]

    def pass_on(what, t, wave, ref, along, d):
        send(("own", wave), (what, wave), ref, ref, flat_dev(along[t], d))

    def send_second(t, wave, j):
        for d in (1, -1):
            pass_on(("second", j), t, wave, block(t, wave, j, 0), seconds, d)

    def gather_1(wave):
        receive(("first", wave), both(wave, 2))
        for t in (0, 1):
            for d in (1, -1):
                pass_on("first half", t, wave, block(t, wave, -d, 0, 0 if d == 1 else 1), firsts, d)
        for j in (-1, 1):
            for t in (0, 1):
                send_second(t, wave, j)

    def gather_2(wave):
        receive(("first half", wave), both(wave, 1))
        for t in (0, 1):
            send_second(t, wave, 2)

    def gather_3(wave, j):
        receive((("second", j), wave), both(wave, 2))
        if wave != TAKE:
            for t in (0, 1):
                for d in (1, -1):
                    pass_on("second half", t, wave, block(t, wave, j, -d, 0 if d == 1 else 1), seconds, d)

    def relay():
        for t in (0, 1):
            for d in (1, -1):
                g = (g_at[t] + 2) % RING
                rows = pl.ds(pl.multiple_of((g * RING + (0 if d == 1 else 2)) * BLOCK, BLOCK), 2 * BLOCK)
                send(
                    "relay",
                    ("second half", TAKE),
                    weights[GIVE].at[t, rows, :],
                    weights[TAKE].at[t, rows, :],
                    z_dev(2 * d),
                )

    def gather_4(wave):
        receive(("second half", wave), both(wave, 4))

    barrier = pltpu.get_barrier_semaphore()
    around = [flat_dev("x", 1), flat_dev("x", -1), flat_dev("y", 1), flat_dev("y", -1), z_dev(1), z_dev(-1)]
    around += [z_dev(2), z_dev(-2)]
    for device in around:
        pl.semaphore_signal(barrier, inc=1, device_id=device, device_id_type=MESH)
    loads = []
    for wave in range(len(WAVES)):
        for t in (0, 1):
            start = pl.multiple_of(half * (WIDTH // 2) + columns_at(wave) + t * WAVES[wave], 128)
            loads.append(
                pltpu.make_async_copy(
                    w_hbm.at[:, pl.ds(start, WAVES[wave])], block(t, wave, 0, 0), local_sem.at[wave]
                )
            )
    k_load = pltpu.make_async_copy(k_hbm, k_in, local_sem.at[len(WAVES)])
    v_load = pltpu.make_async_copy(v_hbm, v_in, local_sem.at[len(WAVES) + 1])
    q_load = pltpu.make_async_copy(q_hbm, k_in, local_sem.at[len(WAVES) + 2])
    for load in loads[:2] + [k_load, v_load] + loads[2:]:
        load.start()
    pl.semaphore_wait(barrier, len(around))

    def send_own(wave):
        ref = both(wave, 1)
        pltpu.make_async_copy(ref, ref, local_sem.at[wave]).wait()
        for t in (0, 1):
            for d in (1, -1):
                pass_on("first", t, wave, block(t, wave, 0, 0), firsts, d)
        for t in (0, 1):
            send_second(t, wave, 0)

    LOTS = ((0, 32), (32, 32), (64, 64))
    SOON = LOTS[0][1]

    def near_row(d, lot):
        start, count = LOTS[lot]
        return NEAR - start - count if d == 1 else NEAR + start

    def near_rows(d, lot):
        return near.at[pl.ds(near_row(d, lot) * HEADS, LOTS[lot][1] * HEADS), :]

    def send_queries(lot):
        for d in (1, -1):
            start, count = LOTS[lot]
            position = TOKENS - start - count if d == 1 else start
            send(
                "q",
                ("q", lot),
                q_hbm.at[pl.ds(position * HEADS, count * HEADS), :],
                near_rows(d, lot),
                z_dev(d),
            )

    send_own(0)
    send_own(GIVE)
    send_queries(0)

    def widen(src, at, count, fn):
        def step(i, carry):
            for u in range(4):
                row = pl.multiple_of((i * 4 + u) * HEADS, HEADS)
                to = pl.multiple_of((at + i * 4 + u) * PITCH, 8)
                wide[pl.ds(to, HEADS), :] = fn(src(row))
            return carry

        lax.fori_loop(0, count // 4, step, 0)

    def as_feature(values):
        return feature(values.astype(F32)).astype(BF16).astype(F32)

    k_load.wait()
    widen(lambda row: k_in[pl.ds(row, HEADS), :], 0, TOKENS, as_feature)
    q_load.start()
    v_load.wait()
    widen(lambda row: v_in[pl.ds(row, HEADS), :], TOKENS, TOKENS, lambda values: values.astype(F32))

    sub = lax.broadcasted_iota(jnp.int32, (8, SIZE), 0)

    def states(i, carry):
        masses = []
        for u in (0, 1):
            head = 2 * i + u
            keys = wide[pl.ds(head, TOKENS, stride=PITCH), :]
            values = wide[pl.ds(TOKENS * PITCH + head, TOKENS, stride=PITCH), :]
            part[i, pl.ds(u * SIZE, SIZE), :] = lax.dot_general(
                keys.astype(BF16), values.astype(BF16), (((0,), (0,)), ((), ())), preferred_element_type=F32
            )
            masses.append(jnp.sum(keys, axis=0, keepdims=True))
        part[i, pl.ds(2 * SIZE, 8), :] = jnp.where(sub == 0, masses[0], jnp.where(sub == 1, masses[1], 0.0))
        return carry

    lax.fori_loop(0, PAIRS, states, 0)

    def at(chunk, u):
        return ((chunk + 2 * DEPTH) % DEPTH) * 2 + u

    lands = {1: from_left, -1: from_right}

    def reduce_send(d, step, u):
        send("sum", ("sum", d, step, u), part.at[at(z + d * (5 - step), u)], lands[d].at[2 * (step - 1) + u], z_dev(d))

    def reduce_add(d, step, u):
        slot = 2 * (step - 1) + u
        receive(("sum", d, step, u), lands[d].at[slot])
        mine = at(z + d * (4 - step), u)
        part[mine] = part[mine] + lands[d][slot]

    def widen_queries(lot):
        receive(("q", lot), near.at[pl.ds(0, 2 * LOTS[lot][1] * HEADS), :])
        for d in (1, -1):
            row = near_row(d, lot)
            widen(lambda at, row=row: near[pl.ds(row * HEADS + at, HEADS), :], row, LOTS[lot][1], as_feature)

    for d, u in ((1, 0), (-1, 1)):
        reduce_send(d, 1, u)
    for d, u in ((1, 1), (-1, 0)):
        reduce_send(d, 2, u)
    gather_1(0)

    q_load.wait()
    widen(lambda row: k_in[pl.ds(row, HEADS), :], OWN, TOKENS, as_feature)
    widen_queries(0)

    def reduce_step(step, u):
        for d in (1, -1):
            v = u if d == 1 else 1 - u
            reduce_add(d, step, v)
            reduce_send(d, step + 1, v)

    def gather_send(d, step, u):
        ref = held.at[at(z - d * (step - 1), u)]
        send("state", ("state", d, step, u), ref, ref, z_dev(d))

    def gather_take(d, step, u):
        receive(("state", d, step, u), held.at[at(z - d * step, u)])

    def read_pair(i, blocks):
        terms = held[i, pl.ds(2 * SIZE, 16), :].astype(F32)
        block_at = i
        other_at = (i % RING) * RING + i // RING
        for u in (0, 1):
            head = 2 * i + u
            mass = terms[u : u + 1] + terms[2 + u : 3 + u] + terms[4 + u : 5 + u]
            state = held[i, pl.ds(u * SIZE, SIZE), :]
            for r, count in blocks:
                ask = wide[pl.ds(r * PITCH + head, count, stride=PITCH), :]
                bottom = jnp.sum(ask * mass, axis=1, keepdims=True) + 0.001
                top = jnp.dot(ask.astype(BF16), state, preferred_element_type=F32)
                result = (top * (2048.0**0.5 / bottom)).astype(BF16)
                for t, b in ((0, block_at), (1, other_at)):
                    to = pl.multiple_of(b * BLOCK + u * SIZE, SIZE)
                    mixed[t, pl.ds(r, count), pl.ds(to, SIZE)] = result

    EARLY = ((NEAR - SOON, 2 * SOON), (OWN, TOKENS))
    LATE = ((0, NEAR - SOON), (NEAR + SOON, NEAR - SOON))

    def read_pairs(first, count, blocks):
        def step(j, carry):
            read_pair(first + j, blocks)
            return carry

        lax.fori_loop(0, count, step, 0)

    def read_chunk(chunk):
        read_pairs(at(chunk, 0), 2, EARLY)

    def own_sums():
        mine = at(z, 0)
        for u in (0, 1):
            for d in (1, -1):
                receive(("sum", d, 4, u), lands[d].at[6 + u])
            total = (part[mine + u] + from_left[6 + u] + from_right[6 + u]) * (1.0 / 2048.0)
            held[mine + u, pl.ds(0, 2 * SIZE), :] = total[: 2 * SIZE].astype(BF16)
            mass = total[2 * SIZE :]
            high = mass.astype(BF16).astype(F32)
            middle = (mass - high).astype(BF16).astype(F32)
            low = mass - high - middle
            terms = high + pltpu.roll(middle, 2, axis=0) + pltpu.roll(low, 4, axis=0)
            terms = jnp.concatenate([terms, jnp.zeros_like(low)], axis=0)
            held[mine + u, pl.ds(2 * SIZE, 16), :] = terms.astype(BF16)
            for d in (1, -1):
                gather_send(d, 1, u)

    def gather_step(step):
        for u in (0, 1):
            for d in (1, -1):
                if step < 4 or (u == 0) == (d == 1):
                    gather_take(d, step, u)
                    if step < 3 or (step == 3 and (u == 0) == (d == 1)):
                        gather_send(d, step + 1, u)

    def read_step(step):
        for d in (1, -1) if step < 4 else (1,):
            read_chunk(z - d * step)

    def finish(wave):
        columns = pl.ds(pl.multiple_of(half * (WIDTH // 2) + columns_at(wave), 128), 2 * WAVES[wave])
        for d, row, to in ((-1, 0, NEAR), (1, NEAR, 0)):
            send(
                ("out", wave),
                ("out", wave),
                done[wave].at[pl.ds(row, NEAR), :],
                out.at[pl.ds(to, NEAR), columns],
                z_dev(d),
            )

    def multiply(wave, rows_at, groups, first, last):
        for t in (0, 1):

            def step(start, tile, n, carry, t=t):
                column = pl.multiple_of(start + n * tile, tile)
                to = pl.multiple_of(t * WAVES[wave] + start + n * tile, 128)
                rows = pl.ds(rows_at, 256)
                total = None if first else acc[rows, pl.ds(to, tile)]
                for dg in groups:
                    g = (g_at[t] + dg + RING) % RING
                    depth = pl.ds(pl.multiple_of(g * RING * BLOCK, RING * BLOCK), RING * BLOCK)
                    product = jnp.dot(
                        mixed[t, rows, depth], weights[wave][t, depth, pl.ds(column, tile)], preferred_element_type=F32
                    )
                    total = product if total is None else total + product
                if not last:
                    acc[rows, pl.ds(to, tile)] = total
                elif rows_at == 0:
                    done[wave][:, pl.ds(to, tile)] = total.astype(BF16)
                else:
                    at = pl.multiple_of(half * (WIDTH // 2) + columns_at(wave) + to, 128)
                    out[:, pl.ds(at, tile)] = total.astype(BF16)
                return carry

            pairs, rest = divmod(WAVES[wave], 256)
            if pairs:
                lax.fori_loop(0, pairs, functools.partial(step, 0, 256), 0)
            if rest:
                step(pairs * 256, rest, 0, 0)

    WHOLE = (0, -1, 1, 2)

    def near_products(wave):
        multiply(wave, 0, WHOLE, True, True)
        finish(wave)

    def own_products(wave):
        multiply(wave, OWN, WHOLE, True, True)

    gather_3(0, 0)
    for d, u in ((1, 0), (-1, 1)):
        reduce_add(d, 1, u)
        reduce_send(d, 2, u)
    gather_1(1)
    reduce_step(2, 1)
    reduce_step(2, 0)
    send_own(3)
    reduce_step(3, 1)
    reduce_step(3, 0)
    send_queries(2)
    own_sums()
    gather_2(1)
    gather_3(1, 0)
    gather_1(3)
    gather_2(0)
    gather_3(1, 2)
    gather_3(1, -1)
    send_own(2)
    read_chunk(z)
    gather_step(1)
    gather_3(1, 1)
    send_queries(1)
    gather_step(2)
    gather_3(0, 1)
    gather_1(2)
    gather_step(3)
    read_step(1)
    gather_2(3)
    gather_3(0, -1)
    gather_3(0, 2)
    read_step(2)
    widen_queries(1)
    widen_queries(2)
    gather_4(1)
    gather_3(3, -1)
    read_step(3)
    relay()
    gather_step(4)
    gather_3(3, 1)
    send_own(4)
    read_step(4)
    own_products(1)
    read_pairs(0, PAIRS, LATE)
    near_products(1)
    gather_3(2, 1)
    gather_3(3, 0)
    gather_3(3, 2)
    gather_4(0)
    own_products(0)
    gather_1(4)
    near_products(0)
    gather_2(4)
    gather_4(3)
    gather_3(2, -1)
    gather_2(2)
    gather_3(4, 0)
    gather_3(2, 0)
    gather_3(4, -1)
    near_products(3)
    own_products(3)
    gather_3(4, 1)
    gather_3(4, 2)
    multiply(4, 0, (0, -1, 1), True, False)
    gather_4(2)
    gather_3(2, 2)
    near_products(2)
    own_products(2)
    gather_4(4)
    multiply(4, 0, (2,), False, True)
    finish(4)
    multiply(4, OWN, (0, -1, 1), True, False)
    multiply(4, OWN, (2,), False, True)

    for wave in range(len(WAVES)):
        all_sent(("own", wave), both(wave, 11 if wave == TAKE else 15))
    all_sent("relay", both(GIVE, 4))
    all_sent("q", near)
    all_sent("sum", part.at[pl.ds(0, 14)])
    all_sent("state", held.at[pl.ds(0, 14)])
    for wave in range(len(WAVES)):
        all_sent(("out", wave), done[wave])
    for wave in range(len(WAVES)):
        receive(("out", wave), done[wave])
    assert len(send_ids) <= SENDS and len(ids) <= RECEIVES, (len(send_ids), len(ids))


SENDS = 14
RECEIVES = 72


def body(query_rows, key_rows, value_rows, out_weight):
    rows = [a.reshape(TOKENS * HEADS, SIZE) for a in (query_rows, key_rows, value_rows)]
    anywhere = pl.BlockSpec(memory_space=pltpu.HBM)
    result = pl.pallas_call(
        kernel,
        out_shape=pltpu.VMEM((TOKENS, WIDTH), BF16),
        in_specs=[anywhere] * 4,
        out_specs=pl.BlockSpec(memory_space=pltpu.VMEM),
        scratch_shapes=[pltpu.VMEM((2, WIDTH, columns), BF16) for columns in WAVES]
        + [pltpu.VMEM((ROWS, 2 * columns), F32) for columns in WAVES[-1:]]
        + [pltpu.VMEM((OWN, 2 * columns), BF16) for columns in WAVES]
        + [
            pltpu.VMEM((TOKENS * HEADS, SIZE), BF16),
            pltpu.VMEM((TOKENS * HEADS, SIZE), BF16),
            pltpu.VMEM((OWN * HEADS, SIZE), BF16),
            pltpu.VMEM((ROWS * PITCH, SIZE), F32),
            pltpu.VMEM((PAIRS, SUMS, SIZE), F32),
            pltpu.VMEM((8, SUMS, SIZE), F32),
            pltpu.VMEM((8, SUMS, SIZE), F32),
            pltpu.VMEM((PAIRS, SENT, SIZE), BF16),
            pltpu.VMEM((2, ROWS, WIDTH), BF16),
            pltpu.SemaphoreType.DMA((len(WAVES) + 3,)),
            pltpu.SemaphoreType.DMA((SENDS,)),
            pltpu.SemaphoreType.DMA((RECEIVES,)),
        ],
        compiler_params=pltpu.CompilerParams(
            collective_id=0, has_side_effects=True, vmem_limit_bytes=56 * 1024 * 1024
        ),
        name="attend",
    )(*rows, out_weight)
    return result.reshape(1, TOKENS, WIDTH)


def solution(mesh):
    placed = (
        P(("shift", "dp"), "sp", None, None),
        P(("shift", "dp"), "sp", None, None),
        P(("shift", "dp"), "sp", None, None),
        P(("shift", "dp"), None),
    )
    return jax.shard_map(
        body, mesh=mesh, in_specs=placed, out_specs=P(("shift", "dp"), "sp", None), check_vma=False
    )
```
